32 devices in a mesh: row: 8 (over z, y), col: 4 (over x, core).
Axes of the slice: x: 2, y: 2, z: 4, core: 2. Of those that a mesh axis runs over, the one named last changes fastest.
Arguments:
- valence: bfloat16 [32768, 2048], P('row', 'col')
- conduction: bfloat16 [32768, 1024], P('row', 'col')
- point_index: int32 [8192], replicated, may hold values from 0 to 32767, as said below
Outputs:
- gram: float32 [8192, 8192], P('col', 'row')
The draws below stay inside these ranges and needn't reach their ends.
Inputs may be any that keep to these rules, and one draw needn't show every extreme that they name: `point_index`: 8192 distinct cells; cell g lies in slab g // 4096. In each aligned block of 1024 entries, at most 256 lie in any one slab, and in every block some slab holds exactly 256.
All inputs are finite; a program needn't handle non-finite values.
Results may differ from the reference program's by a relative error of at most 0.0003.
Values may be sent and summed in bfloat16 or wider, within the bound.
A program may use at most 128 MiB of HBM per device.

```python
import jax
import jax.numpy as jnp
from jax import lax

NV = 2048
NC = 1024
NP = 8192
GRID_DEV = 4096
PR = 1024
CAP = 256
N_ROW = 8


mode_count = 16


def orbital_draw(key, rows, bands):
    noise_key, coef_key, mode_key = jax.random.split(key, 3)
    noise = jax.random.normal(noise_key, (rows, bands), jnp.float32)
    coefs = 0.5 * jax.random.normal(coef_key, (rows, mode_count), jnp.float32)
    modes = jax.random.normal(mode_key, (mode_count, bands), jnp.float32)
    values = (noise + jnp.dot(coefs, modes)) / jnp.sqrt(5.0 * bands)
    return values.astype(jnp.bfloat16)


def draw_valence(key, part):
    return orbital_draw(key, GRID_DEV * N_ROW, NV)


def draw_conduction(key, part):
    return orbital_draw(jax.random.fold_in(key, 11), GRID_DEV * N_ROW, NC)


def draw_point_index(key, part):
    slots = N_ROW * CAP
    score_key, favor_key, cell_key, order_key = jax.random.split(key, 4)
    scores = jax.random.randint(score_key, (N_ROW, slots), 0, 1 << 16) * slots
    scores = scores + jnp.arange(slots, dtype=jnp.int32)[None, :]
    favored = jax.random.randint(favor_key, (N_ROW,), 0, N_ROW)
    slot_slab = jnp.arange(slots, dtype=jnp.int32) // CAP
    scores = scores + jnp.where(slot_slab[None, :] == favored[:, None], 1 << 29, 0)
    chosen = lax.top_k(scores, PR)[1].astype(jnp.int32)
    slab = chosen // CAP
    within = chosen - slab * CAP
    perms = jax.vmap(lambda k: jax.random.permutation(k, GRID_DEV))(jax.random.split(cell_key, N_ROW)).astype(jnp.int32)
    block_ids = jnp.arange(N_ROW, dtype=jnp.int32)[:, None]
    local = perms[slab, block_ids * CAP + within]
    cells = slab * GRID_DEV + local
    orders = jax.vmap(lambda k: jax.random.permutation(k, PR))(jax.random.split(order_key, N_ROW)).astype(jnp.int32)
    cells = jnp.take_along_axis(cells, orders, axis=1)
    return cells.reshape(NP).astype(jnp.int32)


def setup_inputs(seed: int = 0) -> dict:
    key_of = jax.random.split(jax.random.key(seed), 4)
    return {
        "valence": draw_valence(jax.random.fold_in(key_of[3], 71), 0),
        "conduction": draw_conduction(jax.random.fold_in(key_of[3], 71), 0),
        "point_index": draw_point_index(jax.random.fold_in(key_of[3], 71), 0),
    }


def full_total(rows, cols):
    left = rows.astype(jnp.float32)
    right = cols.astype(jnp.float32)
    return jnp.dot(left, right.T, precision=lax.Precision.HIGHEST)


def reference(valence, conduction, point_index):
    psi_mu = jnp.take(valence, point_index, axis=0)
    phi_mu = jnp.take(conduction, point_index, axis=0)
    psi_blocks = psi_mu.reshape(NP // PR, PR, NV)
    phi_blocks = phi_mu.reshape(NP // PR, PR, NC)

    def one_block(pair):
        return full_total(pair[0], psi_mu) * full_total(pair[1], phi_mu)

    stacked = lax.map(one_block, (psi_blocks, phi_blocks))
    return stacked.reshape(NP, NP)
```

```python
import functools

import jax
import jax.numpy as jnp
from jax import lax
from jax.experimental import pallas as pl
from jax.experimental.pallas import tpu as pltpu
from jax.sharding import PartitionSpec as P

MESH = pl.DeviceIdType.MESH
CHUNK_ROWS = 16
GROUP = 8
COLUMN_TILE = 256


def spread_kernel(
    n, c, wv, w, half,
    x_ref, o_ref, own, full, own_sem, peer_send, peer_recv, mate_send, mate_recv, ring_send, ring_recv,
):
    span = n // c
    pairs = c // 2
    chunks = half // CHUNK_ROWS
    stage_rows = half // GROUP
    group_rows = GROUP * CHUNK_ROWS
    row, col = lax.axis_index("row"), lax.axis_index("col")
    core, chip = lax.rem(col, 2), col // 2
    mate = chip * 2 + 1 - core

    def position(r):
        y, z = lax.rem(r, 2), r // 2
        return (1 - y) * z + y * (n - 1 - z)

    def row_at(p):
        back = p // (n // 2)
        return (1 - back) * (2 * p) + back * (2 * (n - 1 - p) + 1)

    here = position(row)
    right, left = row_at(lax.rem(here + 1, n)), row_at(lax.rem(here + n - 1, n))

    barrier = pltpu.get_barrier_semaphore()
    for other in (left, right):
        pl.semaphore_signal(barrier, inc=1, device_id=(other, col), device_id_type=MESH)
    for q in range(1, c):
        pl.semaphore_signal(
            barrier, inc=1, device_id=(row, lax.rem(col + q, c)), device_id_type=MESH
        )

    def piece(owner, first, count):
        return own.at[pl.ds(first, count), pl.ds(pl.multiple_of(owner * w, 128), w)]

    mine = pltpu.make_async_copy(x_ref, piece(col, 0, 2 * half), own_sem)
    mine.start()
    pl.semaphore_wait(barrier, 2 + c - 1)
    mine.wait()

    def stage_first(m, h):
        return pl.multiple_of(h * half + m * stage_rows, stage_rows)

    def to_peer(q, owner, m, h):
        ref = piece(owner, stage_first(m, h), stage_rows)
        return pltpu.make_async_remote_copy(
            src_ref=ref, dst_ref=ref,
            send_sem=peer_send.at[q - 1], recv_sem=peer_recv.at[q - 1, m, h],
            device_id=(row, lax.rem(chip + q, pairs) * 2 + core), device_id_type=MESH,
        )

    def to_mate(q, owner, m, h):
        ref = piece(owner, stage_first(m, h), stage_rows)
        return pltpu.make_async_remote_copy(
            src_ref=ref, dst_ref=ref,
            send_sem=mate_send.at[q], recv_sem=mate_recv.at[q, m, h],
            device_id=(row, mate), device_id_type=MESH,
        )

    def send_own(m, _):
        for h in range(2):
            for q in range(1, pairs):
                to_peer(q, col, m, h).start()
            to_mate(0, col, m, h).start()
        return 0

    lax.fori_loop(0, GROUP, send_own, 0)

    def stream(i, t):
        s, back = i // 2, lax.rem(i, 2)
        source = position(span * col + s)
        distance = lax.rem((1 - back) * (here - source) + back * (source - here) + n, n)
        return s, back, distance, t - distance

    def ring_copy(i, k, s, back, source_ref, source_first):
        first = pl.multiple_of(s * 2 * half + back * half + k * CHUNK_ROWS, CHUNK_ROWS)
        return pltpu.make_async_remote_copy(
            src_ref=source_ref.at[pl.ds(pl.multiple_of(source_first, CHUNK_ROWS), CHUNK_ROWS)],
            dst_ref=full.at[pl.ds(first, CHUNK_ROWS)],
            send_sem=ring_send.at[i], recv_sem=ring_recv.at[i, k],
            device_id=((1 - back) * right + back * left, col), device_id_type=MESH,
        )

    def step(t, _):
        @pl.when(t < GROUP)
        def _():
            for h in range(2):
                for q in range(1, pairs):
                    owner = lax.rem(chip - q + pairs, pairs) * 2 + core
                    to_peer(q, owner, t, h).wait_recv()
                    to_mate(q, owner, t, h).start()
            for h in range(2):
                for q in range(pairs):
                    owner = lax.rem(chip - q + pairs, pairs) * 2 + 1 - core
                    to_mate(q, owner, t, h).wait_recv()

        def forward(i, _):
            s, back, distance, k = stream(i, t)

            @pl.when((k >= 0) & (k < chunks))
            def _():
                in_block = back * half + k * CHUNK_ROWS

                @pl.when(distance == 0)
                def _():
                    ring_copy(i, k, s, back, own, in_block).start()

                @pl.when(distance > 0)
                def _():
                    copy = ring_copy(i, k, s, back, full, s * 2 * half + in_block)
                    copy.wait_recv()

                    @pl.when(distance < n - 1)
                    def _():
                        copy.start()

            return 0

        lax.fori_loop(0, 2 * span, forward, 0)

        def compute(i, _):
            s, back, distance, k = stream(i, t)

            @pl.when((k >= 0) & (k < chunks) & (lax.rem(k + GROUP, GROUP) == GROUP - 1))
            def _():
                in_block = pl.multiple_of(
                    back * half + (k - (GROUP - 1)) * CHUNK_ROWS, group_rows
                )
                first = pl.multiple_of(s * 2 * half + in_block, group_rows)

                @pl.when(distance == 0)
                def _():
                    full[pl.ds(first, group_rows), :] = own[pl.ds(in_block, group_rows), :]

                def tile(j, _):
                    begin = pl.multiple_of(j * COLUMN_TILE, COLUMN_TILE)
                    totals = []
                    for low, high in ((0, wv), (wv, w)):
                        total = None
                        for p in range(c):
                            part = lax.dot_general(
                                full[pl.ds(first, group_rows), p * w + low : p * w + high],
                                own[pl.ds(begin, COLUMN_TILE), p * w + low : p * w + high],
                                (((1,), (1,)), ((), ())),
                                preferred_element_type=jnp.float32,
                            )
                            total = part if total is None else total + part
                        totals.append(total)
                    o_ref[pl.ds(first, group_rows), pl.ds(begin, COLUMN_TILE)] = totals[0] * totals[1]
                    return 0

                lax.fori_loop(0, 2 * half // COLUMN_TILE, tile, 0)

            return 0

        lax.fori_loop(0, 2 * span, compute, 0)
        return 0

    lax.fori_loop(0, chunks + n - 1, step, 0)

    whole = piece(col, 0, 2 * half)
    for q in range(pairs):
        if q >= 1:
            pltpu.make_async_copy(whole, whole, peer_send.at[q - 1]).wait()
        pltpu.make_async_copy(whole, whole, mate_send.at[q]).wait()

    def drain(i, _):
        distance = stream(i, 0)[2]

        @pl.when(distance < n - 1)
        def _():
            stretch = full.at[pl.ds(0, half)]
            pltpu.make_async_copy(stretch, stretch, ring_send.at[i]).wait()

        return 0

    lax.fori_loop(0, 2 * span, drain, 0)


def spread_and_multiply(x, wv, n, c):
    points, w = x.shape
    span = n // c
    half = points // 2
    chunks = half // CHUNK_ROWS
    pairs = c // 2
    return pl.pallas_call(
        functools.partial(spread_kernel, n, c, wv, w, half),
        out_shape=jax.ShapeDtypeStruct((span * points, points), jnp.float32),
        in_specs=[pl.BlockSpec(memory_space=pl.ANY)],
        out_specs=pl.BlockSpec(memory_space=pltpu.VMEM),
        scratch_shapes=[
            pltpu.VMEM((points, c * w), jnp.bfloat16),
            pltpu.VMEM((span * points, c * w), jnp.bfloat16),
            pltpu.SemaphoreType.DMA,
            pltpu.SemaphoreType.DMA((max(pairs - 1, 1),)),
            pltpu.SemaphoreType.DMA((max(pairs - 1, 1), GROUP, 2)),
            pltpu.SemaphoreType.DMA((pairs,)),
            pltpu.SemaphoreType.DMA((pairs, GROUP, 2)),
            pltpu.SemaphoreType.DMA((2 * span,)),
            pltpu.SemaphoreType.DMA((2 * span, chunks)),
        ],
        compiler_params=pltpu.CompilerParams(
            collective_id=0, has_side_effects=True, vmem_limit_bytes=48 * 1024 * 1024
        ),
    )(x)


def on_device(valence, conduction, point_index):
    row_count = lax.axis_size("row")
    col_count = lax.axis_size("col")
    my_row = lax.axis_index("row")
    grid_cells = valence.shape[0]
    total_points = point_index.shape[0]
    block_points = total_points // row_count
    capacity = max(2 * block_points // row_count, 2)
    blocks = point_index.reshape(row_count, block_points)
    owners = blocks // grid_cells
    offsets = blocks - owners * grid_cells
    onehot = owners[:, None, :] == jnp.arange(row_count, dtype=jnp.int32)[None, :, None]
    place = jnp.arange(block_points, dtype=jnp.int32)
    earlier = (place[:, None] < place[None, :]).astype(jnp.bfloat16)
    before = lax.dot_general(
        onehot.astype(jnp.bfloat16), earlier, (((2,), (0,)), ((), ())),
        preferred_element_type=jnp.float32,
    )
    ranks = jnp.sum(jnp.where(onehot, before, 0.0), axis=1).astype(jnp.int32)
    owned = owners == my_row
    picked = owned[:, None, :] & (
        ranks[:, None, :] == jnp.arange(capacity, dtype=jnp.int32)[None, :, None]
    )
    source_cells = jnp.sum(jnp.where(picked, offsets[:, None, :], 0), axis=2)
    own_owner = lax.dynamic_index_in_dim(owners, my_row, 0, keepdims=False)
    own_rank = lax.dynamic_index_in_dim(ranks, my_row, 0, keepdims=False)
    flat_slot = own_owner * capacity + own_rank

    def route(array):
        send = array.at[source_cells].get(mode="promise_in_bounds")
        got = lax.all_to_all(send, "row", split_axis=0, concat_axis=0, tiled=True)
        got = got.reshape(row_count * capacity, got.shape[2])
        return got.at[flat_slot].get(mode="promise_in_bounds")

    rows = jnp.concatenate([route(valence), route(conduction)], axis=1)
    return spread_and_multiply(rows, valence.shape[1], row_count, col_count)


def solution(mesh):
    placed = (P("row", "col"), P("row", "col"), P())
    return jax.shard_map(
        on_device, mesh=mesh, in_specs=placed, out_specs=P("col", "row"), check_vma=False
    )
```

```python
import functools

import jax
import jax.numpy as jnp
from jax import lax
from jax.experimental import pallas as pl
from jax.experimental.pallas import tpu as pltpu
from jax.sharding import PartitionSpec as P

MESH = pl.DeviceIdType.MESH
CHUNK_ROWS = 16
GROUP = 8
COLUMN_TILE = 256


def spread_kernel(
    n, c, wv, w, half,
    x_ref, o_ref, own, full, own_sem, peer_send, peer_recv, mate_send, mate_recv, ring_send, ring_recv,
):
    span = n // c
    pairs = c // 2
    chunks = half // CHUNK_ROWS
    stage_rows = half // GROUP
    group_rows = GROUP * CHUNK_ROWS
    stride = GROUP // (2 * half // COLUMN_TILE)
    row, col = lax.axis_index("row"), lax.axis_index("col")
    core, chip = lax.rem(col, 2), col // 2
    mate = chip * 2 + 1 - core

    def position(r):
        y, z = lax.rem(r, 2), r // 2
        return (1 - y) * z + y * (n - 1 - z)

    def row_at(p):
        back = p // (n // 2)
        return (1 - back) * (2 * p) + back * (2 * (n - 1 - p) + 1)

    here = position(row)
    right, left = row_at(lax.rem(here + 1, n)), row_at(lax.rem(here + n - 1, n))

    barrier = pltpu.get_barrier_semaphore()
    for other in (left, right):
        pl.semaphore_signal(barrier, inc=1, device_id=(other, col), device_id_type=MESH)
    for q in range(1, c):
        pl.semaphore_signal(
            barrier, inc=1, device_id=(row, lax.rem(col + q, c)), device_id_type=MESH
        )

    def piece(owner, first, count):
        return own.at[pl.ds(first, count), pl.ds(pl.multiple_of(owner * w, 128), w)]

    mine = pltpu.make_async_copy(x_ref, piece(col, 0, 2 * half), own_sem)
    mine.start()
    pl.semaphore_wait(barrier, 2 + c - 1)
    mine.wait()

    def stage_first(m, h):
        return pl.multiple_of(h * half + m * stage_rows, stage_rows)

    def to_peer(q, owner, m, h):
        ref = piece(owner, stage_first(m, h), stage_rows)
        return pltpu.make_async_remote_copy(
            src_ref=ref, dst_ref=ref,
            send_sem=peer_send.at[q - 1], recv_sem=peer_recv.at[q - 1, m, h],
            device_id=(row, lax.rem(chip + q, pairs) * 2 + core), device_id_type=MESH,
        )

    def to_mate(q, owner, m, h):
        ref = piece(owner, stage_first(m, h), stage_rows)
        return pltpu.make_async_remote_copy(
            src_ref=ref, dst_ref=ref,
            send_sem=mate_send.at[q], recv_sem=mate_recv.at[q, m, h],
            device_id=(row, mate), device_id_type=MESH,
        )

    def send_own(m, _):
        for h in range(2):
            for q in range(1, pairs):
                to_peer(q, col, m, h).start()
            to_mate(0, col, m, h).start()
        return 0

    lax.fori_loop(0, GROUP, send_own, 0)

    def stream(i, t):
        s, back = i // 2, lax.rem(i, 2)
        source = position(span * col + s)
        distance = lax.rem((1 - back) * (here - source) + back * (source - here) + n, n)
        return s, back, distance, t - distance

    def ring_copy(i, k, s, back, source_ref, source_first):
        first = pl.multiple_of(s * 2 * half + back * half + k * CHUNK_ROWS, CHUNK_ROWS)
        return pltpu.make_async_remote_copy(
            src_ref=source_ref.at[pl.ds(pl.multiple_of(source_first, CHUNK_ROWS), CHUNK_ROWS)],
            dst_ref=full.at[pl.ds(first, CHUNK_ROWS)],
            send_sem=ring_send.at[i], recv_sem=ring_recv.at[i, k],
            device_id=((1 - back) * right + back * left, col), device_id_type=MESH,
        )

    def step(t, _):
        @pl.when(t < GROUP)
        def _():
            for h in range(2):
                for q in range(1, pairs):
                    owner = lax.rem(chip - q + pairs, pairs) * 2 + core
                    to_peer(q, owner, t, h).wait_recv()
                    to_mate(q, owner, t, h).start()
            for h in range(2):
                for q in range(pairs):
                    owner = lax.rem(chip - q + pairs, pairs) * 2 + 1 - core
                    to_mate(q, owner, t, h).wait_recv()

        def forward(i, _):
            s, back, distance, k = stream(i, t)

            @pl.when((k >= 0) & (k < chunks))
            def _():
                in_block = back * half + k * CHUNK_ROWS

                @pl.when(distance == 0)
                def _():
                    ring_copy(i, k, s, back, own, in_block).start()

                @pl.when(distance > 0)
                def _():
                    copy = ring_copy(i, k, s, back, full, s * 2 * half + in_block)
                    copy.wait_recv()

                    @pl.when(distance < n - 1)
                    def _():
                        copy.start()

            return 0

        lax.fori_loop(0, 2 * span, forward, 0)

        def compute(i, _):
            s, back, distance, k = stream(i, t)
            since = k - (GROUP - 1)
            phase = lax.rem(since + GROUP, GROUP)

            @pl.when((since >= 0) & (since < chunks) & (lax.rem(phase, stride) == 0))
            def _():
                in_block = pl.multiple_of(back * half + (since - phase) * CHUNK_ROWS, group_rows)
                first = pl.multiple_of(s * 2 * half + in_block, group_rows)
                begin = pl.multiple_of(phase // stride * COLUMN_TILE, COLUMN_TILE)

                @pl.when((distance == 0) & (phase == 0))
                def _():
                    full[pl.ds(first, group_rows), :] = own[pl.ds(in_block, group_rows), :]

                totals = []
                for low, high in ((0, wv), (wv, w)):
                    total = None
                    for p in range(c):
                        part = lax.dot_general(
                            full[pl.ds(first, group_rows), p * w + low : p * w + high],
                            own[pl.ds(begin, COLUMN_TILE), p * w + low : p * w + high],
                            (((1,), (1,)), ((), ())),
                            preferred_element_type=jnp.float32,
                        )
                        total = part if total is None else total + part
                    totals.append(total)
                o_ref[pl.ds(first, group_rows), pl.ds(begin, COLUMN_TILE)] = totals[0] * totals[1]

            return 0

        lax.fori_loop(0, 2 * span, compute, 0)
        return 0

    lax.fori_loop(0, chunks + n - 1 + GROUP - 1, step, 0)

    whole = piece(col, 0, 2 * half)
    for q in range(pairs):
        if q >= 1:
            pltpu.make_async_copy(whole, whole, peer_send.at[q - 1]).wait()
        pltpu.make_async_copy(whole, whole, mate_send.at[q]).wait()

    def drain(i, _):
        distance = stream(i, 0)[2]

        @pl.when(distance < n - 1)
        def _():
            stretch = full.at[pl.ds(0, half)]
            pltpu.make_async_copy(stretch, stretch, ring_send.at[i]).wait()

        return 0

    lax.fori_loop(0, 2 * span, drain, 0)


def spread_and_multiply(x, wv, n, c):
    points, w = x.shape
    span = n // c
    half = points // 2
    chunks = half // CHUNK_ROWS
    pairs = c // 2
    return pl.pallas_call(
        functools.partial(spread_kernel, n, c, wv, w, half),
        out_shape=pltpu.VMEM((span * points, points), jnp.float32),
        in_specs=[pl.BlockSpec(memory_space=pl.ANY)],
        out_specs=pl.BlockSpec(memory_space=pltpu.VMEM),
        scratch_shapes=[
            pltpu.VMEM((points, c * w), jnp.bfloat16),
            pltpu.VMEM((span * points, c * w), jnp.bfloat16),
            pltpu.SemaphoreType.DMA,
            pltpu.SemaphoreType.DMA((max(pairs - 1, 1),)),
            pltpu.SemaphoreType.DMA((max(pairs - 1, 1), GROUP, 2)),
            pltpu.SemaphoreType.DMA((pairs,)),
            pltpu.SemaphoreType.DMA((pairs, GROUP, 2)),
            pltpu.SemaphoreType.DMA((2 * span,)),
            pltpu.SemaphoreType.DMA((2 * span, chunks)),
        ],
        compiler_params=pltpu.CompilerParams(
            collective_id=0, has_side_effects=True, vmem_limit_bytes=32 * 1024 * 1024
        ),
    )(x)


def on_device(valence, conduction, point_index):
    row_count = lax.axis_size("row")
    col_count = lax.axis_size("col")
    my_row = lax.axis_index("row")
    grid_cells = valence.shape[0]
    total_points = point_index.shape[0]
    block_points = total_points // row_count
    capacity = max(2 * block_points // row_count, 2)
    blocks = point_index.reshape(row_count, block_points)
    owners = blocks // grid_cells
    offsets = blocks - owners * grid_cells
    onehot = owners[:, None, :] == jnp.arange(row_count, dtype=jnp.int32)[None, :, None]
    place = jnp.arange(block_points, dtype=jnp.int32)
    earlier = (place[:, None] < place[None, :]).astype(jnp.bfloat16)
    before = lax.dot_general(
        onehot.astype(jnp.bfloat16), earlier, (((2,), (0,)), ((), ())),
        preferred_element_type=jnp.float32,
    )
    ranks = jnp.sum(jnp.where(onehot, before, 0.0), axis=1).astype(jnp.int32)
    owned = owners == my_row
    picked = owned[:, None, :] & (
        ranks[:, None, :] == jnp.arange(capacity, dtype=jnp.int32)[None, :, None]
    )
    source_cells = jnp.sum(jnp.where(picked, offsets[:, None, :], 0), axis=2)
    own_owner = lax.dynamic_index_in_dim(owners, my_row, 0, keepdims=False)
    own_rank = lax.dynamic_index_in_dim(ranks, my_row, 0, keepdims=False)
    flat_slot = own_owner * capacity + own_rank

    def route(array):
        send = array.at[source_cells].get(mode="promise_in_bounds")
        got = lax.all_to_all(send, "row", split_axis=0, concat_axis=0, tiled=True)
        got = got.reshape(row_count * capacity, got.shape[2])
        return got.at[flat_slot].get(mode="promise_in_bounds")

    rows = jnp.concatenate([route(valence), route(conduction)], axis=1)
    return spread_and_multiply(rows, valence.shape[1], row_count, col_count)


def solution(mesh):
    placed = (P("row", "col"), P("row", "col"), P())
    return jax.shard_map(
        on_device, mesh=mesh, in_specs=placed, out_specs=P("col", "row"), check_vma=False
    )
```
